256 devices in a mesh: groups: 4 (over y, x), gx: 32 (over z), gy: 2 (over core).
Axes of the slice: x: 2, y: 2, z: 32, core: 2. Of those that a mesh axis runs over, the one named last changes fastest.
The devices are a block of a 4x8x32 slice.
Arguments:
- tokens: bfloat16 [2, 8192, 7168], P(None, ('groups', 'gx', 'gy')), parts along dimension 1, may hold values from -6 to 6
- expert_ids: int32 [2, 8192, 2], P(None, ('groups', 'gx', 'gy')), parts along dimension 1, may hold values from 0 to 15, all different within a row; in each aligned block of 32 rows (0 to 31, 32 to 63, ..., all dimensions but the last counted through in order) at most 6 rows name the same one
- gate_weights: float32 [2, 8192, 2], P(None, ('groups', 'gx', 'gy')), parts along dimension 1, may hold values from 0.1 to 1
- w_gate: bfloat16 [32, 7168, 512], P('gx', None, 'gy'), may hold values from -0.0625 to 0.0625
- w_up: bfloat16 [32, 7168, 512], P('gx', None, 'gy'), may hold values from -0.0625 to 0.0625
- w_down: bfloat16 [32, 512, 7168], P('gx', 'gy'), may hold values from -0.1875 to 0.1875
Outputs:
- combined: bfloat16 [2, 8192, 7168], P(None, ('groups', 'gx', 'gy')), parts along dimension 1
The draws below stay inside these ranges and needn't reach their ends.
There are 4 independent parts, one for each index of `groups`. The reference program is written for one: setup_inputs(seed, part) draws one part's arguments, and reference() takes and returns one part's arrays. A program takes and returns all parts, laid end to end along the dimension named above; an argument that names none is the same for every part. Nothing has to cross between parts.
Inputs may be any that keep to these rules, and one draw needn't show every extreme that they name: `expert_ids`: each row names 2 different experts. Within the 32 rows of one device and one micro-batch no expert is named more than 6 times, and in some such blocks one is named exactly 6 times.
All inputs are finite; a program needn't handle non-finite values.
Results may differ from the reference program's by a relative error of at most 0.012.
Values may be sent and summed in bfloat16 or wider, within the bound.
A program may use at most 192 MiB of HBM per device.

```python
import math
import jax
import jax.numpy as jnp
import numpy as np
from jax import lax

D = 7168
FFW = 1024
TOPK = 2
MB = 2
ROWS = 32
EXPERTS = 16
CAP = 6
TOKENS = 2048
N_GX = 32
N_GY = 2


def steps_of(rng, dims, shards, low, top_value):
    gain, own = 1.0, jax.random.fold_in(rng, 6)
    for axis_at, blocks in shards:
        steps = jnp.exp(jax.random.uniform(jax.random.fold_in(own, axis_at), (blocks,), jnp.float32, low / len(shards), top_value / len(shards)))
        gain = gain * jnp.repeat(steps, dims[axis_at] // blocks).reshape([-1 if axis == axis_at else 1 for axis in range(len(dims))])
    return gain


def shared_out(stream_key, own, number, rows, count, top, most, lean):
    ranking = jax.random.permutation(stream_key, count)
    packed, ordinary = shares(count, rows * top, most, lean, True), shares(count, rows * top, most, lean, False)
    places = jnp.arange(count)

    def named(sizes, rotation):
        used = int((sizes > 0).sum())
        fixed = max(1, used // 4)
        passed = fixed + (places - fixed + rotation * (used - fixed)) % max(1, count - fixed)
        return jnp.zeros((count,), jnp.int32).at[ranking[jnp.where(places < fixed, places, passed)]].set(jnp.asarray(sizes, jnp.int32))

    sizes = jnp.where(number % 4 == 0, named(packed, number // 4), named(ordinary, number - number // 4 - 1))
    mixed = jax.random.permutation(jax.random.fold_in(own, 3), count)
    source_of, sink = mixed[0:count // 2 * 2:2], mixed[1:count // 2 * 2:2]
    margin = jnp.minimum(sizes[source_of] - 1, most - sizes[sink]) // 2
    margin = jnp.where((source_of == ranking[0]) | (sink == ranking[0]) | (sizes[sink] == 0), 0, jnp.maximum(margin, 0))
    passed = jax.random.randint(jax.random.fold_in(own, 4), (count // 2,), 0, 1 << 20) % (margin + 1)
    sizes = sizes.at[source_of].add(-passed).at[sink].add(passed)
    labels = jnp.searchsorted(jnp.cumsum(sizes), jnp.arange(rows * top), side="right").astype(jnp.int32)
    table = labels.reshape(top, rows).T
    table = table[jax.random.permutation(jax.random.fold_in(own, 1), rows)]
    rotation = jax.random.randint(jax.random.fold_in(own, 2), (rows, 1), 0, top)
    return jnp.take_along_axis(table, (jnp.arange(top)[None, :] + rotation) % top, axis=1)


def shares(amount, total, most, lean, full):
    portions = [(1 << 20) // math.isqrt(standing ** lean) + 1 for standing in range(1, amount + 1)]
    largest = most if full else min(most, max(-(-total // amount), total * portions[0] // sum(portions)))
    least = 1 if total - largest >= amount - 1 else 0
    given, surplus = [largest] + [least] * (amount - 1), total - largest - least * (amount - 1)
    while surplus > 0:
        candidates = [i for i in range(1, amount) if given[i] < largest] or [i for i in range(1, amount) if given[i] < most]
        pool, remaining = sum([portions[i] for i in candidates]), surplus
        for i in candidates:
            addition = min(most - given[i], max(1, remaining * portions[i] // pool), surplus)
            given[i] = given[i] + addition
            surplus = surplus - addition
    return np.array(given)


def scatter_about(stream_key, extent, deviation, most, split=(), kind=jnp.bfloat16):
    factor_of = steps_of(stream_key, extent, split, -0.22, 0.18) if split else 1.0
    drawn = jax.random.normal(stream_key, extent, jnp.float32) * deviation * factor_of
    return jnp.minimum(jnp.maximum(drawn, -most), most).astype(kind)


def setup_inputs(seed: int = 0, part: int = 0) -> dict:
    keys = jax.random.split(jax.random.key(seed), 7)
    part_splits = jax.random.split(jax.random.fold_in(keys[6], part), 7)
    tokens = scatter_about(part_splits[0], (MB, TOKENS, D), 1.0, 6.0, ((1, 64),))
    expert_ids_keys = jax.random.split(jax.random.fold_in(part_splits[1], 1), MB * TOKENS // ROWS)
    expert_ids_turns = jax.random.permutation(jax.random.fold_in(part_splits[1], 3), MB * TOKENS // ROWS)
    expert_ids = jax.vmap(lambda own, number: shared_out(jax.random.fold_in(part_splits[1], 2), own, number, ROWS, EXPERTS, TOPK, CAP, 1))(expert_ids_keys, expert_ids_turns).reshape((MB, TOKENS, TOPK))
    gate_weights = jnp.clip(jnp.exp(math.log(1.0) - 2.3025851 * jax.random.uniform(part_splits[2], (MB, TOKENS, TOPK), jnp.float32) ** steps_of(part_splits[2], (MB, TOKENS, TOPK), ((1, 64),), -0.2, 0.2)), 0.1, 1.0)
    w_gate = scatter_about(keys[3], (2 * EXPERTS, D, FFW // 2), D ** -0.5, 0.0625, ((0, 32), (2, 2)))
    w_up = scatter_about(keys[4], (2 * EXPERTS, D, FFW // 2), D ** -0.5, 0.0625, ((0, 32), (2, 2)))
    w_down = scatter_about(keys[5], (2 * EXPERTS, FFW // 2, D), FFW ** -0.5, 0.1875, ((0, 32), (1, 2)))
    return dict(tokens=tokens, expert_ids=expert_ids, gate_weights=gate_weights, w_gate=w_gate, w_up=w_up, w_down=w_down)


def reference(tokens, expert_ids, gate_weights, w_gate, w_up, w_down):
    devices = N_GX * N_GY
    quarter = FFW // (2 * N_GY)
    ids = expert_ids.reshape(MB, devices, ROWS * TOPK)
    marks = (ids[..., None] == jnp.arange(EXPERTS, dtype=jnp.int32)).astype(jnp.int32)
    before = jnp.cumsum(marks, axis=2) - marks
    slot = jnp.sum(before * marks, axis=-1).reshape(MB, devices, ROWS, TOPK)
    chosen = ids.reshape(MB, devices, ROWS, TOPK)
    token_rows = tokens.reshape(MB, devices, ROWS, D).astype(jnp.float32)
    gates = gate_weights.reshape(MB, devices, ROWS, TOPK).astype(jnp.float32)
    slot_iota = jnp.arange(CAP, dtype=jnp.int32)

    def one_expert(total, inputs):
        index, wg, wu, wd = inputs
        hit = ((chosen == index)[..., None] & (slot[..., None] == slot_iota)).astype(jnp.float32)
        pick = jnp.sum(hit, axis=3)
        mixing = jnp.sum(hit * gates[..., None], axis=3)
        buffer = jnp.einsum("mdrc,mdrf->mdcf", pick, token_rows).astype(jnp.bfloat16).reshape(-1, D)
        halves = []
        for half_index in range(2):
            summed = jnp.zeros((buffer.shape[0], D), jnp.float32)
            for slice_index in range(N_GY):
                low = slice_index * quarter
                gate = jnp.dot(buffer, wg[half_index][:, low:low + quarter], preferred_element_type=jnp.float32)
                up = jnp.dot(buffer, wu[half_index][:, low:low + quarter], preferred_element_type=jnp.float32)
                hidden = (jax.nn.silu(gate) * up).astype(jnp.bfloat16)
                partial_value = jnp.dot(hidden, wd[half_index][low:low + quarter, :], preferred_element_type=jnp.float32)
                summed = summed + partial_value.astype(jnp.bfloat16).astype(jnp.float32)
            halves.append(summed.astype(jnp.bfloat16).astype(jnp.float32))
        expert_out = (halves[0] + halves[1]).reshape(MB, devices, CAP, D)
        total = total + jnp.einsum("mdrc,mdcf->mdrf", mixing, expert_out, precision=lax.Precision.HIGHEST)
        return total, None

    start = jnp.zeros((MB, devices, ROWS, D), jnp.float32)
    inputs = (jnp.arange(EXPERTS, dtype=jnp.int32),
              w_gate.reshape(EXPERTS, 2, D, FFW // 2),
              w_up.reshape(EXPERTS, 2, D, FFW // 2),
              w_down.reshape(EXPERTS, 2, FFW // 2, D))
    total, unused = lax.scan(one_expert, start, inputs)
    return total.astype(jnp.bfloat16).reshape(MB, devices * ROWS, D)
```

```python
import functools

import jax
import jax.numpy as jnp
from jax import lax
from jax.experimental import pallas as pl
from jax.experimental.pallas import tpu as pltpu
from jax.sharding import PartitionSpec as P

MESH = pl.DeviceIdType.MESH
CHUNKS = 4
GROUP = 16


class Ring:
    def __init__(self, n, batches, rows, capacity):
        self.n = n
        self.hops = n // 2
        self.whole = n // 4
        self.experts = n // 2
        self.batches = batches
        self.tokens = batches * rows
        self.capacity = capacity
        self.used = batches * capacity
        assert self.used <= GROUP

    def listed(self, hop):
        return (self.hops - hop) // 2 + 1

    def sent(self, hop):
        if hop <= self.whole:
            return self.tokens
        return -(-self.listed(hop) * self.used // 8) * 8

    @property
    def most(self):
        return self.sent(self.whole + 1)

    def place(self, me, way):
        return me if way == 0 else self.n - 1 - me

    def source(self, me, way, hop):
        return lax.rem(self.place(me, way) - hop + self.n, self.n)

    def first(self, me, way, hop):
        start = self.source(me, way, hop)
        return (start + self.hops - 1) // 2 - (start + hop) // 2

    def group(self, way, hop):
        if hop == self.hops or way == 0:
            return hop
        return self.hops + hop

    def target(self, row, expert):
        batch = jnp.zeros_like(row)
        for b in range(1, self.batches):
            batch = batch + (row >= b * self.capacity).astype(jnp.int32)
        key = batch * (self.experts * self.capacity - self.capacity) + row + expert * self.capacity
        return jnp.where(row < self.used, key, -1).astype(jnp.float32)

    def list_target(self, row, me, way, hop):
        start = self.source(me, way, hop)
        last = lax.rem((start + self.hops - 1) // 2, self.experts)
        at = jnp.zeros_like(row)
        for k in range(1, self.listed(self.whole + 1)):
            at = at + (row >= k * self.used).astype(jnp.int32)
        expert = last - at
        expert = jnp.where(expert < 0, expert + self.experts, expert)
        if way == 1:
            expert = self.experts - 1 - expert
        row = row - at * self.used
        return jnp.where(
            at < self.listed(self.whole + 1), self.target(row, expert), -1.0
        )


def iota(shape, dim):
    return lax.broadcasted_iota(jnp.int32, shape, dim)


def enter(right, left):
    barrier = pltpu.get_barrier_semaphore()
    for neighbour in (left, right):
        pl.semaphore_signal(barrier, inc=1, device_id={"gx": neighbour}, device_id_type=MESH)
    pl.semaphore_wait(barrier, 2)


def columns(c, width):
    return pl.ds(c * width, width)


def dispatch_kernel(ring, x_ref, meta_ref, rows_ref, metas_ref, tok, slots, conv,
                    send_sem, recv_sem, meta_send, meta_recv):
    n, hops, whole = ring.n, ring.hops, ring.whole
    me = lax.axis_index("gx")
    right, left = lax.rem(me + 1, n), lax.rem(me + n - 1, n)
    width = x_ref.shape[1]
    part = width // CHUNKS
    expert = me // 2

    def held(way, hop):
        if hop == 0:
            return x_ref
        if hop <= whole:
            return tok.at[way, hop - 1]
        return slots.at[way, hop - whole - 1]

    def copy(way, hop, c):
        source = conv.at[way] if hop == whole + 1 else held(way, hop - 1)
        rows = pl.ds(0, ring.sent(hop))
        return pltpu.make_async_remote_copy(
            src_ref=source.at[rows, columns(c, part)],
            dst_ref=held(way, hop).at[rows, columns(c, part)],
            send_sem=send_sem.at[way, hop - 1, c],
            recv_sem=recv_sem.at[way, hop - 1, c],
            device_id={"gx": left if way else right},
            device_id_type=MESH,
        )

    def meta_copy(way, hop):
        return pltpu.make_async_remote_copy(
            src_ref=meta_ref if hop == 1 else metas_ref.at[way, hop - 2],
            dst_ref=metas_ref.at[way, hop - 1],
            send_sem=meta_send.at[way, hop - 1],
            recv_sem=meta_recv.at[way, hop - 1],
            device_id={"gx": left if way else right},
            device_id_type=MESH,
        )

    def picker(meta, target):
        keys = [meta[k : k + 1, : ring.tokens] for k in range(2)]
        hit = (keys[0] == target) | (keys[1] == target)
        return hit.astype(jnp.float32).astype(jnp.bfloat16)

    def spread(parts, group):
        @pl.loop(0, CHUNKS)
        def _(c):
            at = pl.ds(pl.multiple_of(c * part, 128), part)
            total = None
            for pick, block, count in parts:
                value = jnp.dot(pick, block[pl.ds(0, count), at], preferred_element_type=jnp.float32)
                total = value if total is None else total + value
            rows_ref[pl.ds(group * GROUP, GROUP), at] = total.astype(jnp.bfloat16)

    own_target = ring.target(iota((GROUP, 1), 0), expert)

    enter(right, left)
    for way in range(2):
        meta_copy(way, 1).start()
    for c in range(CHUNKS):
        for way in range(2):
            copy(way, 1, c).start()
    spread([(picker(meta_ref[...], own_target), x_ref, ring.tokens)], 0)

    for hop in range(1, hops + 1):
        for way in range(2):
            meta_copy(way, hop).wait_recv()
            if hop < hops:
                meta_copy(way, hop + 1).start()
        if hop == whole:
            pickers = [
                picker(
                    metas_ref[way, hop - 1],
                    ring.list_target(iota((ring.most, 1), 0), me, way, hop),
                )
                for way in range(2)
            ]
        for c in range(CHUNKS):
            for way in range(2):
                copy(way, hop, c).wait_recv()
                if hop == whole:
                    conv[way, :, columns(c, part)] = jnp.dot(
                        pickers[way],
                        tok[way, whole - 1, :, columns(c, part)],
                        preferred_element_type=jnp.float32,
                    ).astype(jnp.bfloat16)
                if hop < hops:
                    copy(way, hop + 1, c).start()
        parts = []
        for way in range(2):
            if hop <= whole:
                pick = picker(metas_ref[way, hop - 1], own_target)
            else:
                first = ring.first(me, way, hop)
                shape = (GROUP, ring.sent(hop))
                row, col = iota(shape, 0), iota(shape, 1)
                hit = (col == first * ring.used + row) & (row < ring.used) & (row >= -first * GROUP)
                pick = hit.astype(jnp.float32).astype(jnp.bfloat16)
            parts.append((pick, held(way, hop), ring.sent(hop)))
        if hop == hops:
            spread(parts, hop)
        else:
            for way in range(2):
                spread(parts[way : way + 1], ring.group(way, hop))

    for hop in range(1, hops + 1):
        for way in range(2):
            meta_copy(way, hop).wait_send()
            for c in range(CHUNKS):
                copy(way, hop, c).wait_send()


def return_kernel(ring, y_ref, metas_ref, out_ref, tok, slots, turn, last, send_sem, recv_sem):
    n, hops, whole = ring.n, ring.hops, ring.whole
    me = lax.axis_index("gx")
    right, left = lax.rem(me + 1, n), lax.rem(me + n - 1, n)
    width = out_ref.shape[1]
    part = width // CHUNKS
    expert = me // 2

    def held(way, hop):
        if hop < whole:
            return tok.at[way, hop]
        if hop < hops:
            return slots.at[way, hop - whole]
        return last.at[way]

    def copy(way, hop, c):
        rows = pl.ds(0, ring.sent(hop))
        source = turn.at[way] if hop == whole else held(way, hop)
        return pltpu.make_async_remote_copy(
            src_ref=source.at[rows, columns(c, part)],
            dst_ref=held(way, hop - 1).at[rows, columns(c, part)],
            send_sem=send_sem.at[way, hop - 1, c],
            recv_sem=recv_sem.at[way, hop - 1, c],
            device_id={"gx": right if way else left},
            device_id_type=MESH,
        )

    def mixer(at, target):
        meta = metas_ref[at]
        mix = jnp.zeros((ring.tokens, target.shape[1]), jnp.float32)
        for k in range(2):
            mix = mix + jnp.where(meta[:, k : k + 1] == target, meta[:, 2 + k : 3 + k], 0.0)
        high = mix.astype(jnp.bfloat16)
        return high, (mix - high.astype(jnp.float32)).astype(jnp.bfloat16)

    def mixed(pair, rows):
        return jnp.dot(pair[0], rows, preferred_element_type=jnp.float32) + jnp.dot(
            pair[1], rows, preferred_element_type=jnp.float32
        )

    def own_rows(way, hop, c):
        return y_ref[pl.ds(ring.group(way, hop) * GROUP, GROUP), columns(c, part)]

    def placer(way, hop):
        first = ring.first(me, way, hop)
        shape = (ring.sent(hop), GROUP)
        row, col = iota(shape, 0), iota(shape, 1)
        hit = (row == first * ring.used + col) & (col < ring.used) & (col >= -first * GROUP)
        return hit.astype(jnp.float32).astype(jnp.bfloat16)

    for hop in range(whole + 1, hops):
        more, had = ring.sent(hop), ring.sent(hop + 1)
        if more > had:
            for way in range(2):
                slots[way, hop - whole, pl.ds(had, more - had), :] = jnp.zeros(
                    (more - had, width), jnp.bfloat16
                )

    enter(right, left)
    own_target = ring.target(iota((1, GROUP), 1), expert)
    for hop in range(hops, 0, -1):
        count = ring.sent(hop)
        if hop > whole:
            tables = [placer(way, hop) for way in range(2)]
        else:
            tables = [mixer(way * (whole + 1) + hop, own_target) for way in range(2)]
        if hop == whole:
            lists = [
                mixer(
                    way * (whole + 1) + hop,
                    ring.list_target(iota((1, ring.most), 1), me, way, hop),
                )
                for way in range(2)
            ]
        for c in range(CHUNKS):
            for way in range(2):
                at = columns(c, part)
                if hop < hops:
                    copy(way, hop + 1, c).wait_recv()
                rows = own_rows(way, hop, c)
                if hop > whole:
                    value = jnp.dot(tables[way], rows, preferred_element_type=jnp.float32)
                    if hop == hops:
                        last[way, :, at] = value.astype(jnp.bfloat16)
                    else:
                        have = slots[way, hop - whole, pl.ds(0, count), at]
                        slots[way, hop - whole, pl.ds(0, count), at] = (
                            value + have.astype(jnp.float32)
                        ).astype(jnp.bfloat16)
                elif hop == whole:
                    value = mixed(tables[way], rows) + mixed(lists[way], slots[way, 0, :, at])
                    turn[way, :, at] = value.astype(jnp.bfloat16)
                else:
                    value = mixed(tables[way], rows) + tok[way, hop, :, at].astype(jnp.float32)
                    tok[way, hop, :, at] = value.astype(jnp.bfloat16)
                copy(way, hop, c).start()
    own = mixer(0, own_target)
    for c in range(CHUNKS):
        at = columns(c, part)
        value = mixed(own, own_rows(0, 0, c))
        for way in range(2):
            copy(way, 1, c).wait_recv()
            value = value + tok[way, 0, :, at].astype(jnp.float32)
        out_ref[:, at] = value.astype(jnp.bfloat16)
    for hop in range(1, hops + 1):
        for way in range(2):
            for c in range(CHUNKS):
                copy(way, hop, c).wait_send()


def vmem(count=1):
    return [pl.BlockSpec(memory_space=pltpu.VMEM)] * count


def dispatch(ring, tokens, meta):
    width = tokens.shape[1]
    groups = ring.n
    hops, whole = ring.hops, ring.whole
    sems = pltpu.SemaphoreType.DMA
    sent = sum(ring.sent(hop) for hop in range(1, hops + 1)) * width * 4
    return pl.pallas_call(
        functools.partial(dispatch_kernel, ring),
        out_shape=(
            jax.ShapeDtypeStruct((groups * GROUP, width), jnp.bfloat16),
            jax.ShapeDtypeStruct((2, hops, 8, 128), jnp.float32),
        ),
        in_specs=vmem(2),
        out_specs=tuple(vmem(2)),
        scratch_shapes=[
            pltpu.VMEM((2, whole, ring.tokens, width), jnp.bfloat16),
            pltpu.VMEM((2, hops - whole, ring.most, width), jnp.bfloat16),
            pltpu.VMEM((2, ring.most, width), jnp.bfloat16),
            sems((2, hops, CHUNKS)),
            sems((2, hops, CHUNKS)),
            sems((2, hops)),
            sems((2, hops)),
        ],
        compiler_params=pltpu.CompilerParams(collective_id=0, has_side_effects=True),
        cost_estimate=pl.CostEstimate(
            flops=4 * groups * GROUP * 64 * width, bytes_accessed=20 * sent, transcendentals=0
        ),
        name="dispatch",
    )(tokens, meta)


def give_back(ring, values, metas, width):
    hops, whole = ring.hops, ring.whole
    sems = pltpu.SemaphoreType.DMA
    sent = sum(ring.sent(hop) for hop in range(1, hops + 1)) * width * 4
    return pl.pallas_call(
        functools.partial(return_kernel, ring),
        out_shape=jax.ShapeDtypeStruct((ring.tokens, width), jnp.bfloat16),
        in_specs=vmem(2),
        out_specs=vmem()[0],
        scratch_shapes=[
            pltpu.VMEM((2, whole, ring.tokens, width), jnp.bfloat16),
            pltpu.VMEM((2, hops - whole, ring.most, width), jnp.bfloat16),
            pltpu.VMEM((2, ring.tokens, width), jnp.bfloat16),
            pltpu.VMEM((2, ring.sent(hops), width), jnp.bfloat16),
            sems((2, hops, CHUNKS)),
            sems((2, hops, CHUNKS)),
        ],
        compiler_params=pltpu.CompilerParams(collective_id=1, has_side_effects=True),
        cost_estimate=pl.CostEstimate(
            flops=4 * ring.n * GROUP * 64 * width, bytes_accessed=20 * sent, transcendentals=0
        ),
        name="give_back",
    )(values, metas)


def slot_keys(expert_ids, ring):
    batches, rows, topk = expert_ids.shape
    flat = expert_ids.reshape(batches, rows * topk)
    earlier = jnp.tril(jnp.ones((rows * topk, rows * topk), jnp.bool_), -1)
    same = flat[:, :, None] == flat[:, None, :]
    slot = jnp.sum((same & earlier[None]).astype(jnp.int32), axis=2)
    key = flat * ring.capacity + slot
    key = key + jnp.arange(batches, dtype=jnp.int32)[:, None] * (ring.experts * ring.capacity)
    return key.reshape(batches * rows, topk).astype(jnp.float32)


def body(tokens, expert_ids, gate_weights, w_gate, w_up, w_down):
    batches, rows, width = tokens.shape
    topk = expert_ids.shape[2]
    n = lax.axis_size("gx")
    experts = n // 2
    capacity = 2 * min(rows // 2, (5 * rows * topk + 8 * experts - 1) // (8 * experts))
    ring = Ring(n, batches, rows, capacity)

    keys = slot_keys(expert_ids, ring)
    gates = gate_weights.reshape(batches * rows, topk)
    both = jnp.concatenate([keys, gates], axis=1)
    meta = jnp.pad(both.T, ((0, 8 - 2 * topk), (0, 128 - batches * rows)))

    full_gate = lax.all_gather(w_gate[0], "gy")
    full_up = lax.all_gather(w_up[0], "gy")
    full_down = lax.all_gather(w_down[0], "gy")

    slot_rows, metas = dispatch(ring, tokens.reshape(batches * rows, width), meta)

    values = jnp.zeros((slot_rows.shape[0], width), jnp.float32)
    for q in range(full_gate.shape[0]):
        gate = jnp.dot(slot_rows, full_gate[q], preferred_element_type=jnp.float32)
        up = jnp.dot(slot_rows, full_up[q], preferred_element_type=jnp.float32)
        hidden = (jax.nn.silu(gate) * up).astype(jnp.bfloat16)
        values = values + jnp.dot(hidden, full_down[q], preferred_element_type=jnp.float32)
    values = values.astype(jnp.bfloat16)

    near = jnp.swapaxes(metas[:, : ring.whole, : 2 * topk, : ring.tokens], 2, 3)
    near = jnp.concatenate([jnp.broadcast_to(both, (2, 1, *both.shape)), near], axis=1)
    near = near.reshape(-1, *both.shape)
    out = give_back(ring, values, near, width)
    return out.reshape(batches, rows, width)


def solution(mesh):
    placed = (
        P(None, ("groups", "gx", "gy"), None),
        P(None, ("groups", "gx", "gy"), None),
        P(None, ("groups", "gx", "gy"), None),
        P("gx", None, "gy"),
        P("gx", None, "gy"),
        P("gx", "gy", None),
    )
    return jax.shard_map(
        body,
        mesh=mesh,
        in_specs=placed,
        out_specs=P(None, ("groups", "gx", "gy"), None),
        check_vma=False,
    )
```
